32 devices in a mesh: ctx: 8 (over y, x, core), tp: 4 (over z).
Axes of the slice: x: 2, y: 2, z: 4, core: 2. Of those that a mesh axis runs over, the one named last changes fastest.
Arguments:
- hidden_in: bfloat16 [2048, 4096], P(('ctx', 'tp')), may hold values from -6 to 6
- norm_gain: float32 [4096], replicated, may hold values from 0.5 to 1.5
- proj_weight: bfloat16 [4096, 4096], P(None, 'tp'), may hold values from -0.09375 to 0.09375
- conv_in: bfloat16 [2048, 4096], P('ctx', 'tp'), may hold values from -6 to 6
- conv_weight: float32 [4, 4096], P(None, 'tp'), may hold values from -3 to 3
- conv_bias: float32 [4096], P('tp'), may hold values from -3 to 3
- act_grad: bfloat16 [2048, 4096], P('ctx', 'tp'), may hold values from -6 to 6
Outputs:
- hidden_input_gradient: bfloat16 [2048, 4096], P(('ctx', 'tp'))
- norm_gain_gradient: float32 [4096], replicated
- taps_grad: float32 [4, 4096], P(None, 'tp')
- bias_grad: float32 [4096], P('tp')
The draws below stay inside these ranges and needn't reach their ends.
All inputs are finite; a program needn't handle non-finite values.
Results may differ from the reference program's by a relative error of at most 0.013.
Values may be sent and summed in bfloat16 or wider, within the bound.
A program may use at most 64 MiB of HBM per device.

```python
import jax
import jax.numpy as jnp
from jax import lax

D = 4096
INNER_DEV = 1024
TAPS = 4
TOKENS = 2048
INNER = 4096
N_TP = 4


def block_levels(key, extent, pieces, low, largest):
    def one(dim, blocks):
        steps = jax.random.uniform(jax.random.fold_in(jax.random.fold_in(key, 6), dim), (blocks,), jnp.float32, low / len(pieces), largest / len(pieces))
        return jnp.repeat(jnp.exp(steps), extent[dim] // blocks).reshape((-1,) + (1,) * (len(extent) - dim - 1))

    loudness = one(*pieces[0])
    for cut in pieces[1:]:
        loudness = loudness * one(*cut)
    return loudness


def gaussian(key, dims, scale, reach, split=(), kind=jnp.bfloat16):
    factor_of = block_levels(key, dims, split, -0.22, 0.18) if split else 1.0
    values = jax.random.normal(key, dims, jnp.float32) * scale * factor_of
    return jnp.minimum(jnp.maximum(values, -reach), reach).astype(kind)


def setup_inputs(seed: int = 0) -> dict:
    seeds = jax.random.split(jax.random.key(seed), 8)
    hidden_in = gaussian(seeds[0], (TOKENS, D), 1.0, 6.0, ((0, 32),))
    norm_gain = jnp.clip(1.0 + 0.1 * jax.random.normal(seeds[1], (D,), jnp.float32), 0.5, 1.5)
    proj_weight = gaussian(seeds[2], (D, INNER), INNER ** -0.5, 0.09375, ((1, 4),))
    conv_in = gaussian(seeds[3], (TOKENS, INNER), 1.0, 6.0, ((0, 8), (1, 4)))
    conv_weight = gaussian(seeds[4], (TAPS, INNER), 0.5, 3.0, ((1, 4),), jnp.float32)
    conv_bias = gaussian(seeds[5], (INNER,), 0.5, 3.0, ((0, 4),), jnp.float32)
    act_grad = gaussian(seeds[6], (TOKENS, INNER), 1.0, 6.0, ((0, 8), (1, 4)))
    return {"hidden_in": hidden_in, "norm_gain": norm_gain, "proj_weight": proj_weight, "conv_in": conv_in, "conv_weight": conv_weight, "conv_bias": conv_bias, "act_grad": act_grad}


def channel_block(carry, items):
    saved, cotangent, taps, offset, weight = items
    count_tok = saved.shape[0]
    tap_count = taps.shape[0]
    padded = jnp.concatenate([jnp.zeros((tap_count - 1, saved.shape[1]), jnp.float32), saved.astype(jnp.float32)], 0)
    preact = offset[None, :] + sum((taps[index][None, :] * padded[tap_count - 1 - index:tap_count - 1 - index + count_tok] for index in range(tap_count)))
    sigmoid_v = jax.nn.sigmoid(preact)
    pre_grad = cotangent.astype(jnp.float32) * sigmoid_v * (1.0 + preact * (1.0 - sigmoid_v))
    taps_part = jnp.stack([lax.optimization_barrier(jnp.sum(pre_grad * padded[tap_count - 1 - index:tap_count - 1 - index + count_tok], 0)) for index in range(tap_count)], 0)
    bias_part = lax.optimization_barrier(jnp.sum(pre_grad, 0))
    after = jnp.concatenate([pre_grad, jnp.zeros((tap_count - 1, saved.shape[1]), jnp.float32)], 0)
    in_grad = sum((taps[index][None, :] * after[index:index + count_tok] for index in range(tap_count))).astype(jnp.bfloat16)
    part_grad = lax.dot_general(in_grad, weight, (((1,), (1,)), ((), ())), preferred_element_type=jnp.float32).astype(jnp.bfloat16)
    part_grad = lax.optimization_barrier(part_grad)
    carry = carry + part_grad.astype(jnp.float32)
    return (carry, (taps_part, bias_part))

def reference(hidden_in, norm_gain, proj_weight, conv_in, conv_weight, conv_bias, act_grad):
    count_tok = conv_in.shape[0]
    blocks = N_TP
    width = INNER_DEV
    saved = conv_in.reshape(count_tok, blocks, width).transpose(1, 0, 2)
    cotangent = act_grad.reshape(count_tok, blocks, width).transpose(1, 0, 2)
    taps = conv_weight.reshape(TAPS, blocks, width).transpose(1, 0, 2)
    offset = conv_bias.reshape(blocks, width)
    weight = proj_weight.reshape(D, blocks, width).transpose(1, 0, 2)
    start_sum = jnp.zeros((count_tok, D), jnp.float32)
    normalized_gradient, parts = lax.scan(channel_block, start_sum, (saved, cotangent, taps, offset, weight))
    taps_grad = parts[0].transpose(1, 0, 2).reshape(TAPS, blocks * width)
    bias_grad = parts[1].reshape(blocks * width)
    hidden_state = hidden_in.astype(jnp.float32)
    root_mean_square = jnp.sqrt(lax.optimization_barrier(jnp.mean(hidden_state * hidden_state, -1, keepdims=True)) + 1e-05)
    normalized_input = hidden_state / root_mean_square
    norm_gain_gradient = lax.optimization_barrier(jnp.sum(normalized_gradient * normalized_input, 0))
    scaled_gradient = norm_gain[None, :] * normalized_gradient
    mean_correction = lax.optimization_barrier(jnp.mean(scaled_gradient * normalized_input, -1, keepdims=True))
    hidden_input_gradient = ((scaled_gradient - normalized_input * mean_correction) / root_mean_square).astype(jnp.bfloat16)
    return (hidden_input_gradient, norm_gain_gradient, taps_grad, bias_grad)
```

```python
import functools

import jax
import jax.numpy as jnp
from jax import lax
from jax.experimental import pallas as pl
from jax.experimental.pallas import tpu as pltpu
from jax.sharding import PartitionSpec as P

MESH = pl.DeviceIdType.MESH
F32 = jnp.float32
BF16 = jnp.bfloat16
LANES = 128
EDGE = 16
PAD = 8


def chunk_of(rows, most=64):
    return max(r for r in range(EDGE, most + 1, EDGE) if rows % r == 0)


def each(count, body):
    if count <= 8:
        for k in range(1, count):
            body(k)
    else:
        lax.fori_loop(1, count, lambda k, _: (body(k), 0)[1], 0)


def kernel(
    n_ctx, n_tp, slab_w,
    hid_hbm, gain_ref, w_hbm, x_hbm, taps_ref, bias_ref, g_hbm,
    out_hbm, gain_out, taps_out, bias_out,
    hid_v, w_v, x_v, g_v, halo, xf, pg, act, tb, prod, send, recv,
    xh, ng, inv_v, out_v, tb_all, gain_all, gain_tp,
    in_sem, w_sem, out_sem, halo_send, halo_recv, rs_send, rs_recv,
    tb_send, tb_recv, gc_send, gc_recv, gt_send, gt_recv,
):
    ctx = lax.axis_index("ctx")
    tp = lax.axis_index("tp")
    T, C = x_v.shape
    D = w_v.shape[0]
    taps = taps_ref.shape[0]
    rows = T // n_tp
    half = n_tp // 2
    slabs = D // slab_w
    prev_c, next_c = lax.rem(ctx + n_ctx - 1, n_ctx), lax.rem(ctx + 1, n_ctx)
    ring = (lax.rem(tp + 1, n_tp), lax.rem(tp + n_tp - 1, n_tp))

    barrier = pltpu.get_barrier_semaphore()

    def greet_ctx(k):
        pl.semaphore_signal(barrier, inc=1, device_id={"ctx": lax.rem(ctx + k, n_ctx)}, device_id_type=MESH)

    def greet_tp(k):
        pl.semaphore_signal(barrier, inc=1, device_id={"tp": lax.rem(tp + k, n_tp)}, device_id_type=MESH)

    each(n_ctx, greet_ctx)
    each(n_tp, greet_tp)

    x_in = pltpu.make_async_copy(x_hbm, x_v, in_sem.at[0])
    g_in = pltpu.make_async_copy(g_hbm, g_v, in_sem.at[1])
    h_in = pltpu.make_async_copy(hid_hbm, hid_v, in_sem.at[2])
    x_in.start()
    g_in.start()

    def w_copy(j):
        part = pl.ds(pl.multiple_of(j * slab_w, slab_w), slab_w)
        return pltpu.make_async_copy(w_hbm.at[part], w_v.at[part], w_sem.at[j])

    for j in range(slabs):
        w_copy(j).start()
    h_in.start()

    pl.semaphore_wait(barrier, n_ctx + n_tp - 2)

    def remote(src, dst, s_sem, r_sem, **where):
        return pltpu.make_async_remote_copy(
            src_ref=src, dst_ref=dst, send_sem=s_sem, recv_sem=r_sem,
            device_id=where, device_id_type=MESH,
        )

    halos = [
        remote(x_hbm.at[pl.ds(T - EDGE, EDGE)], halo.at[0], halo_send.at[0], halo_recv.at[0], ctx=next_c),
        remote(x_hbm.at[pl.ds(0, EDGE)], halo.at[1], halo_send.at[1], halo_recv.at[1], ctx=prev_c),
        remote(g_hbm.at[pl.ds(0, EDGE)], halo.at[2], halo_send.at[2], halo_recv.at[2], ctx=prev_c),
    ]
    for copy in halos:
        copy.start()

    x_in.wait()
    g_in.wait()

    def fold(v):
        return v.reshape(v.shape[0] // 8, 8, v.shape[1]).sum(0)

    def grad_rows(t0, count, cols, cot):
        xs = [xf[pl.ds(PAD + t0 - k, count), cols] for k in range(taps)]
        pre = bias_ref[:, cols] + sum(taps_ref[pl.ds(k, 1), cols] * xs[k] for k in range(taps))
        s = 0.5 * jnp.tanh(0.5 * pre) + 0.5
        return xs, cot.astype(F32) * s * (1.0 + pre * (1.0 - s))

    def in_rows(t0, count, cols):
        total = sum(taps_ref[pl.ds(k, 1), cols] * pg[pl.ds(t0 + k, count), cols] for k in range(taps))
        act[pl.ds(t0, count), cols] = total.astype(BF16)

    def columns(c):
        return pl.ds(pl.multiple_of(c * LANES, LANES), LANES)

    step = chunk_of(T - EDGE)
    step_in = chunk_of(T - 2 * EDGE)
    tb[...] = jnp.zeros_like(tb)

    def interior(c, _):
        cols = columns(c)
        xf[pl.ds(PAD, T), cols] = x_v[:, cols].astype(F32)
        sums = [jnp.zeros((8, LANES), F32) for _ in range(taps + 1)]
        for t0 in range(EDGE, T, step):
            xs, g = grad_rows(t0, step, cols, g_v[pl.ds(t0, step), cols])
            pg[pl.ds(t0, step), cols] = g
            for k in range(taps):
                sums[k] += fold(g * xs[k])
            sums[taps] += fold(g)
        for k in range(taps + 1):
            tb[pl.ds(k, 1), cols] = jnp.sum(sums[k], 0, keepdims=True)
        for t0 in range(EDGE, T - EDGE, step_in):
            in_rows(t0, step_in, cols)
        return 0

    lax.fori_loop(0, C // LANES, interior, 0)

    for copy in halos:
        copy.wait_recv()
    has_prev = (ctx > 0).astype(F32)
    has_next = (ctx < n_ctx - 1).astype(F32)

    def edges(c, _):
        cols = columns(c)
        xf[pl.ds(0, PAD), cols] = halo[0, :, cols].astype(F32)[EDGE - PAD:] * has_prev
        xf[pl.ds(PAD + T, PAD), cols] = halo[1, :, cols].astype(F32)[:PAD]
        xs, g = grad_rows(0, EDGE, cols, g_v[pl.ds(0, EDGE), cols])
        pg[pl.ds(0, EDGE), cols] = g
        for k in range(taps):
            tb[pl.ds(k, 1), cols] += jnp.sum(fold(g * xs[k]), 0, keepdims=True)
        tb[pl.ds(taps, 1), cols] += jnp.sum(fold(g), 0, keepdims=True)
        _, after = grad_rows(T, PAD, cols, halo[2, :, cols].astype(F32)[:PAD])
        pg[pl.ds(T, PAD), cols] = after * has_next
        in_rows(0, EDGE, cols)
        in_rows(T - EDGE, EDGE, cols)
        return 0

    lax.fori_loop(0, C // LANES, edges, 0)

    tb_all[ctx] = tb[...]

    def tb_copy(k):
        return remote(
            tb_all.at[ctx], tb_all.at[ctx], tb_send.at[k], tb_recv.at[ctx],
            ctx=lax.rem(ctx + k, n_ctx),
        )

    def owner(d, s):
        away = half - s
        return lax.rem(tp + (away if d == 0 else n_tp - away), n_tp)

    def rs_copy(d, s, j):
        return remote(
            send.at[d, s, j], recv.at[d, s, j], rs_send.at[d, s, j], rs_recv.at[d, s, j],
            tp=ring[d],
        )

    def term(d, s, j):
        return prod[j, pl.ds(pl.multiple_of(owner(d, s) * rows, rows), rows), :]

    def first_sends(pair, _):
        for d in range(2):
            j = 2 * pair + d
            w_copy(j).wait()
            part = pl.ds(pl.multiple_of(j * slab_w, slab_w), slab_w)
            prod[j] = lax.dot_general(
                act[...], w_v[part, :], (((1,), (1,)), ((), ())), preferred_element_type=F32
            )
            send[d, 0, j] = term(d, 0, j).astype(BF16)
            rs_copy(d, 0, j).start()
            send[1 - d, 1, j] = term(1 - d, 1, j).astype(BF16)
            rs_copy(1 - d, 1, j).start()
        return 0

    lax.fori_loop(0, slabs // 2, first_sends, 0)
    each(n_ctx, lambda k: tb_copy(k).start())

    h_in.wait()

    def slab_cols(j):
        return pl.ds(pl.multiple_of(j * slab_w, slab_w), slab_w)

    def fold_lanes(v):
        return sum(v[:, i:i + LANES] for i in range(0, v.shape[1], LANES))

    def squares(j, acc):
        h = hid_v[:, slab_cols(j)].astype(F32)
        return acc + fold_lanes(h * h)

    acc = lax.fori_loop(0, slabs, squares, jnp.zeros((rows, LANES), F32))
    inv = lax.rsqrt(jnp.sum(acc, -1, keepdims=True) / D + 1e-05)
    inv_v[...] = jnp.broadcast_to(inv, (rows, LANES))

    def second_sends(pair, _):
        for d in range(2):
            j = 2 * pair + d
            rs_copy(d, 0, j).wait_recv()
            send[d, 1, j] = (term(d, 1, j) + recv[d, 0, j].astype(F32)).astype(BF16)
            rs_copy(d, 1, j).start()
        return 0

    lax.fori_loop(0, slabs // 2, second_sends, 0)

    for s in range(2, half):
        def later_sends(j, _, s=s):
            for d in range(2):
                rs_copy(d, s - 1, j).wait_recv()
                send[d, s, j] = (term(d, s, j) + recv[d, s - 1, j].astype(F32)).astype(BF16)
                rs_copy(d, s, j).start()
            return 0

        lax.fori_loop(0, slabs, later_sends, 0)

    def normalise(j, _):
        xh[j] = hid_v[:, slab_cols(j)].astype(F32) * inv_v[:, :1]
        return 0

    lax.fori_loop(0, slabs, normalise, 0)

    each(n_ctx, lambda k: remote(
        tb_all.at[ctx], tb_all.at[lax.rem(ctx + k, n_ctx)], tb_send.at[k],
        tb_recv.at[lax.rem(ctx + k, n_ctx)], ctx=next_c,
    ).wait_recv())
    total = lax.fori_loop(1, n_ctx, lambda i, t: t + tb_all[i], tb_all[0])
    taps_out[...] = total[:taps]
    bias_out[...] = total[taps:taps + 1]

    last = half - 1

    def finish(j, macc):
        rs_copy(0, last, j).wait_recv()
        rs_copy(1, last, j).wait_recv()
        mine = prod[j, pl.ds(pl.multiple_of(tp * rows, rows), rows), :]
        v = mine + recv[0, last, j].astype(F32) + recv[1, last, j].astype(F32)
        ng[j] = v
        vx = v * xh[j]
        gain_all[ctx, pl.ds(j, 1), :] = jnp.sum(fold(vx), 0, keepdims=True)
        return macc + fold_lanes(vx * gain_ref[:, slab_cols(j)])

    macc = lax.fori_loop(0, slabs, finish, jnp.zeros((rows, LANES), F32))

    def gc_copy(k, slot):
        return remote(
            gain_all.at[slot], gain_all.at[slot], gc_send.at[k], gc_recv.at[slot],
            ctx=lax.rem(ctx + k, n_ctx),
        )

    each(n_ctx, lambda k: gc_copy(k, ctx).start())

    mean = jnp.sum(macc, -1, keepdims=True) / D

    def write(j, _):
        cols = slab_cols(j)
        res = (gain_ref[:, cols] * ng[j] - xh[j] * mean) * inv_v[:, :1]
        out_v[:, cols] = res.astype(BF16)
        return 0

    lax.fori_loop(0, slabs, write, 0)
    out_copy = pltpu.make_async_copy(out_v, out_hbm, out_sem)
    out_copy.start()

    each(n_ctx, lambda k: gc_copy(k, lax.rem(ctx + k, n_ctx)).wait_recv())
    gain_tp[tp] = lax.fori_loop(1, n_ctx, lambda i, t: t + gain_all[i], gain_all[0])

    def gt_copy(k, slot):
        return remote(
            gain_tp.at[slot], gain_tp.at[slot], gt_send.at[k], gt_recv.at[slot],
            tp=lax.rem(tp + k, n_tp),
        )

    each(n_tp, lambda k: gt_copy(k, tp).start())

    for copy in halos:
        copy.wait_send()
    each(n_ctx, lambda k: tb_copy(k).wait_send())
    each(n_ctx, lambda k: gc_copy(k, ctx).wait_send())

    def drain(pair, _):
        for d in range(2):
            rs_copy(d, 0, 2 * pair + d).wait_send()
            for s in range(1, half):
                rs_copy(d, s, 2 * pair).wait_send()
                rs_copy(d, s, 2 * pair + 1).wait_send()
        return 0

    lax.fori_loop(0, slabs // 2, drain, 0)

    each(n_tp, lambda k: gt_copy(k, lax.rem(tp + k, n_tp)).wait_recv())
    gain_sum = sum(gain_tp[i] for i in range(n_tp))
    for j in range(slabs):
        gain_out[:, j * slab_w:(j + 1) * slab_w] = gain_sum[j:j + 1]
    each(n_tp, lambda k: gt_copy(k, tp).wait_send())
    out_copy.wait()


def on_device(n_ctx, n_tp, hidden_in, norm_gain, proj_weight, conv_in, conv_weight, conv_bias, act_grad):
    T, C = conv_in.shape
    D = proj_weight.shape[0]
    rows = hidden_in.shape[0]
    taps = conv_weight.shape[0]
    half = n_tp // 2
    slab_w = D // 8
    slabs = D // slab_w
    hbm = pl.BlockSpec(memory_space=pl.ANY)
    vmem = pl.BlockSpec(memory_space=pltpu.VMEM)
    dma = pltpu.SemaphoreType.DMA
    grad, gain, taps_grad, bias_grad = pl.pallas_call(
        functools.partial(kernel, n_ctx, n_tp, slab_w),
        out_shape=(
            jax.ShapeDtypeStruct((rows, D), BF16),
            jax.ShapeDtypeStruct((1, D), F32),
            jax.ShapeDtypeStruct((taps, C), F32),
            jax.ShapeDtypeStruct((1, C), F32),
        ),
        in_specs=[hbm, vmem, hbm, hbm, vmem, vmem, hbm],
        out_specs=(hbm, vmem, vmem, vmem),
        scratch_shapes=[
            pltpu.VMEM((rows, D), BF16),
            pltpu.VMEM((D, C), BF16),
            pltpu.VMEM((T, C), BF16),
            pltpu.VMEM((T, C), BF16),
            pltpu.VMEM((3, EDGE, C), BF16),
            pltpu.VMEM((T + 2 * PAD, C), F32),
            pltpu.VMEM((T + PAD, C), F32),
            pltpu.VMEM((T, C), BF16),
            pltpu.VMEM((8, C), F32),
            pltpu.VMEM((slabs, T, slab_w), F32),
            pltpu.VMEM((2, half, slabs, rows, slab_w), BF16),
            pltpu.VMEM((2, half, slabs, rows, slab_w), BF16),
            pltpu.VMEM((slabs, rows, slab_w), F32),
            pltpu.VMEM((slabs, rows, slab_w), F32),
            pltpu.VMEM((rows, LANES), F32),
            pltpu.VMEM((rows, D), BF16),
            pltpu.VMEM((n_ctx, 8, C), F32),
            pltpu.VMEM((n_ctx, slabs, slab_w), F32),
            pltpu.VMEM((n_tp, slabs, slab_w), F32),
            dma((3,)),
            dma((slabs,)),
            dma,
            dma((3,)),
            dma((3,)),
            dma((2, half, slabs)),
            dma((2, half, slabs)),
            dma((n_ctx,)),
            dma((n_ctx,)),
            dma((n_ctx,)),
            dma((n_ctx,)),
            dma((n_tp,)),
            dma((n_tp,)),
        ],
        compiler_params=pltpu.CompilerParams(
            collective_id=0, has_side_effects=True, vmem_limit_bytes=60 * 1024 * 1024
        ),
    )(
        hidden_in, norm_gain[None, :], proj_weight, conv_in, conv_weight, conv_bias[None, :], act_grad
    )
    return grad, gain.reshape(-1), taps_grad, bias_grad.reshape(-1)


def solution(mesh):
    return jax.shard_map(
        functools.partial(on_device, mesh.shape["ctx"], mesh.shape["tp"]),
        mesh=mesh,
        in_specs=(
            P(("ctx", "tp"), None),
            P(),
            P(None, "tp"),
            P("ctx", "tp"),
            P(None, "tp"),
            P("tp"),
            P("ctx", "tp"),
        ),
        out_specs=(P(("ctx", "tp"), None), P(), P(None, "tp"), P("tp")),
        check_vma=False,
    )
```

```python
import functools

import jax
import jax.numpy as jnp
from jax import lax
from jax.experimental import pallas as pl
from jax.experimental.pallas import tpu as pltpu
from jax.sharding import PartitionSpec as P

MESH = pl.DeviceIdType.MESH
F32 = jnp.float32
BF16 = jnp.bfloat16
LANES = 128
EDGE = 16
PAD = 8


def chunk_of(rows, most=64):
    return max(r for r in range(EDGE, most + 1, EDGE) if rows % r == 0)


def each(count, body):
    if count <= 8:
        for k in range(1, count):
            body(k)
    else:
        lax.fori_loop(1, count, lambda k, _: (body(k), 0)[1], 0)


def kernel(
    n_ctx, n_tp, slab_w,
    hid_hbm, gain_hbm, w_hbm, x_hbm, taps_hbm, bias_hbm, g_hbm,
    out_hbm, gain_out, taps_out, bias_out,
    hid_v, w_v, x_v, g_v, gain_ref, taps_ref, bias_ref, halo, xf, pg, act_mid, act_edge, tb, prod, send, recv,
    xh, ng, inv_v, out_v, tb_all, gain_all, gain_tp,
    in_sem, w_sem, out_sem, halo_send, halo_recv, rs_send, rs_recv,
    tb_send, tb_recv, gc_send, gc_recv, gt_send, gt_recv,
):
    ctx = lax.axis_index("ctx")
    tp = lax.axis_index("tp")
    T, C = x_v.shape
    D = w_v.shape[0]
    taps = taps_ref.shape[0]
    rows = T // n_tp
    slabs = D // slab_w
    groups, _, per_group, _ = gain_all.shape
    prev_c, next_c = lax.rem(ctx + n_ctx - 1, n_ctx), lax.rem(ctx + 1, n_ctx)
    line = (lax.rem(tp + 1, n_tp), lax.rem(tp + n_tp - 1, n_tp))

    barrier = pltpu.get_barrier_semaphore()

    def greet_ctx(k):
        pl.semaphore_signal(barrier, inc=1, device_id={"ctx": lax.rem(ctx + k, n_ctx)}, device_id_type=MESH)

    def greet_tp(k):
        pl.semaphore_signal(barrier, inc=1, device_id={"tp": lax.rem(tp + k, n_tp)}, device_id_type=MESH)

    each(n_ctx, greet_ctx)
    each(n_tp, greet_tp)

    inputs = [
        pltpu.make_async_copy(src, dst, in_sem.at[i])
        for i, (src, dst) in enumerate([
            (x_hbm, x_v), (taps_hbm, taps_ref), (bias_hbm, bias_ref), (g_hbm, g_v),
            (hid_hbm, hid_v), (gain_hbm, gain_ref),
        ])
    ]
    for copy in inputs[:4]:
        copy.start()

    def w_copy(j):
        part = pl.ds(pl.multiple_of(j * slab_w, slab_w), slab_w)
        return pltpu.make_async_copy(w_hbm.at[part], w_v.at[part], w_sem.at[j])

    for j in range(slabs):
        w_copy(j).start()
    for copy in inputs[4:]:
        copy.start()

    def remote(src, dst, s_sem, r_sem, **where):
        return pltpu.make_async_remote_copy(
            src_ref=src, dst_ref=dst, send_sem=s_sem, recv_sem=r_sem,
            device_id=where, device_id_type=MESH,
        )

    def fold(v):
        return v.reshape(v.shape[0] // 8, 8, v.shape[1]).sum(0)

    def convert(t0, count, cols):
        xf[pl.ds(PAD + t0, count), cols] = x_v[pl.ds(t0, count), cols].astype(F32)

    def grad_rows(t0, count, cols, cot):
        pre = bias_ref[:, cols] + sum(
            taps_ref[pl.ds(k, 1), cols] * xf[pl.ds(PAD + t0 - k, count), cols] for k in range(taps)
        )
        s = 0.5 * jnp.tanh(0.5 * pre) + 0.5
        return cot.astype(F32) * s * (1.0 + pre * (1.0 - s))

    def own_grad(first, stop, cols):
        step = chunk_of(stop - first)
        for t0 in range(first, stop, step):
            pg[pl.ds(t0, step), cols] = grad_rows(t0, step, cols, g_v[pl.ds(t0, step), cols])

    def in_rows(dst, at, first, count, cols):
        step = chunk_of(count)
        for i in range(0, count, step):
            total = sum(
                taps_ref[pl.ds(k, 1), cols] * pg[pl.ds(first + i + k, step), cols] for k in range(taps)
            )
            dst[pl.ds(at + i, step), cols] = total.astype(BF16)

    def columns(c):
        return pl.ds(pl.multiple_of(c * LANES, LANES), LANES)

    for copy in inputs[:4]:
        copy.wait()

    def middle(c, _):
        cols = columns(c)
        convert(rows - EDGE, T - 2 * rows + 2 * EDGE, cols)
        own_grad(rows, T - rows + EDGE, cols)
        in_rows(act_mid, 0, rows, T - 2 * rows, cols)
        return 0

    lax.fori_loop(0, C // LANES, middle, 0)

    pl.semaphore_wait(barrier, n_ctx + n_tp - 2)
    halos = [
        remote(x_hbm.at[pl.ds(T - EDGE, EDGE)], halo.at[0], halo_send.at[0], halo_recv.at[0], ctx=next_c),
        remote(x_hbm.at[pl.ds(0, EDGE)], halo.at[1], halo_send.at[1], halo_recv.at[1], ctx=prev_c),
        remote(g_hbm.at[pl.ds(0, EDGE)], halo.at[2], halo_send.at[2], halo_recv.at[2], ctx=prev_c),
    ]
    for copy in halos:
        copy.start()

    up = [n_tp - 2, n_tp - 1] + list(range(n_tp - 3, 0, -1))
    chunk = (up, [n_tp - 1 - r for r in up])
    begins = (tp == 0, tp == n_tp - 1)

    def sends(d, r):
        return tp < r if d == 0 else tp > r

    def rs_copy(d, r, j):
        return remote(
            send.at[d, r, j], recv.at[d, r, j], rs_send.at[d, r, j], rs_recv.at[d, r, j],
            tp=line[d],
        )

    def term(r, j):
        return prod[j, pl.ds(r * rows, rows), :]

    def begin(p, j):
        for d in range(2):
            r = chunk[d][p]

            @pl.when(begins[d])
            def _():
                send[d, r, j] = term(r, j).astype(BF16)
                rs_copy(d, r, j).start()

    def dot(a, j):
        part = pl.ds(pl.multiple_of(j * slab_w, slab_w), slab_w)
        return lax.dot_general(
            a[...], w_v[part, :], (((1,), (1,)), ((), ())), preferred_element_type=F32
        )

    def middle_dot(j, _):
        w_copy(j).wait()
        prod[j, pl.ds(rows, T - 2 * rows), :] = dot(act_mid, j)
        begin(0, j)
        return 0

    lax.fori_loop(0, slabs, middle_dot, 0)

    for copy in halos:
        copy.wait_recv()
    has_prev = (ctx > 0).astype(F32)
    has_next = (ctx < n_ctx - 1).astype(F32)

    def edges(c, _):
        cols = columns(c)
        xf[pl.ds(0, PAD), cols] = halo[0, :, cols].astype(F32)[EDGE - PAD:] * has_prev
        xf[pl.ds(PAD + T, PAD), cols] = halo[1, :, cols].astype(F32)[:PAD]
        convert(0, rows - EDGE, cols)
        convert(T - rows + EDGE, rows - EDGE, cols)
        own_grad(0, rows, cols)
        own_grad(T - rows + EDGE, T, cols)
        pg[pl.ds(T, PAD), cols] = has_next * grad_rows(T, PAD, cols, halo[2, :, cols].astype(F32)[:PAD])
        in_rows(act_edge, 0, 0, rows, cols)
        in_rows(act_edge, rows, T - rows, rows, cols)
        return 0

    lax.fori_loop(0, C // LANES, edges, 0)

    def edge_dot(j, _):
        both = dot(act_edge, j)
        prod[j, pl.ds(0, rows), :] = both[:rows]
        prod[j, pl.ds(T - rows, rows), :] = both[rows:]
        begin(1, j)
        return 0

    lax.fori_loop(0, slabs, edge_dot, 0)

    def later_begin(j, _, p=2):
        begin(p, j)
        return 0

    for p in range(2, n_tp - 1):
        lax.fori_loop(0, slabs, functools.partial(later_begin, p=p), 0)

    tb[...] = jnp.zeros_like(tb)

    def taps_terms(c, _):
        cols = columns(c)
        sums = [jnp.zeros((8, LANES), F32) for _ in range(taps + 1)]
        step = chunk_of(T)
        for t0 in range(0, T, step):
            g = pg[pl.ds(t0, step), cols]
            for k in range(taps):
                sums[k] += fold(g * xf[pl.ds(PAD + t0 - k, step), cols])
            sums[taps] += fold(g)
        for k in range(taps + 1):
            tb[pl.ds(k, 1), cols] = jnp.sum(sums[k], 0, keepdims=True)
        return 0

    lax.fori_loop(0, C // LANES, taps_terms, 0)
    tb_all[ctx] = tb[...]

    def tb_copy(k, slot):
        return remote(
            tb_all.at[slot], tb_all.at[slot], tb_send.at[k], tb_recv.at[slot],
            ctx=lax.rem(ctx + k, n_ctx),
        )

    each(n_ctx, lambda k: tb_copy(k, ctx).start())

    for copy in inputs[4:]:
        copy.wait()

    def slab_cols(j):
        return pl.ds(pl.multiple_of(j * slab_w, slab_w), slab_w)

    def fold_lanes(v):
        return sum(v[:, i:i + LANES] for i in range(0, v.shape[1], LANES))

    def squares(j, acc):
        h = hid_v[:, slab_cols(j)].astype(F32)
        return acc + fold_lanes(h * h)

    acc = lax.fori_loop(0, slabs, squares, jnp.zeros((rows, LANES), F32))
    inv = lax.rsqrt(jnp.sum(acc, -1, keepdims=True) / D + 1e-05)
    inv_v[...] = jnp.broadcast_to(inv, (rows, LANES))

    def normalise(j, _):
        xh[j] = hid_v[:, slab_cols(j)].astype(F32) * inv_v[:, :1]
        return 0

    lax.fori_loop(0, slabs, normalise, 0)

    def forward(j, _, p=0):
        def one(d):
            r = chunk[d][p]

            @pl.when(sends(d, r) & jnp.logical_not(begins[d]))
            def _():
                rs_copy(d, r, j).wait_recv()
                send[d, r, j] = (term(r, j) + recv[d, r, j].astype(F32)).astype(BF16)
                rs_copy(d, r, j).start()

        one(0)
        one(1)
        return 0

    for p in range(n_tp - 1):
        lax.fori_loop(0, slabs, functools.partial(forward, p=p), 0)

    each(n_ctx, lambda k: tb_copy(k, lax.rem(ctx + k, n_ctx)).wait_recv())
    total = lax.fori_loop(1, n_ctx, lambda i, t: t + tb_all[i], tb_all[0])
    taps_out[...] = total[:taps]
    bias_out[...] = total[taps:taps + 1]

    def gc_copy(g, k, slot):
        return remote(
            gain_all.at[g, slot], gain_all.at[g, slot], gc_send.at[g, k], gc_recv.at[g, slot],
            ctx=lax.rem(ctx + k, n_ctx),
        )

    def gt_copy(g, k, slot):
        return remote(
            gain_tp.at[g, slot], gain_tp.at[g, slot], gt_send.at[g, k], gt_recv.at[g, slot],
            tp=lax.rem(tp + k, n_tp),
        )

    def blocks_summed(g):
        each(n_ctx, lambda k: gc_copy(g, k, lax.rem(ctx + k, n_ctx)).wait_recv())
        gain_tp[g, tp] = lax.fori_loop(1, n_ctx, lambda i, t: t + gain_all[g, i], gain_all[g, 0])
        each(n_tp, lambda k: gt_copy(g, k, tp).start())

    macc = jnp.zeros((rows, LANES), F32)
    for g in range(groups):
        for i in range(per_group):
            j = g * per_group + i
            ng[j] = prod[j, pl.ds(pl.multiple_of(tp * rows, rows), rows), :]

            def arrived(d):
                rs_copy(d, tp, j).wait_recv()
                ng[j] = ng[j] + recv[d, tp, j].astype(F32)

            pl.when(tp < n_tp - 1)(functools.partial(arrived, 1))
            pl.when(tp > 0)(functools.partial(arrived, 0))
            vx = ng[j] * xh[j]
            gain_all[g, ctx, pl.ds(i, 1), :] = jnp.sum(fold(vx), 0, keepdims=True)
            macc = macc + fold_lanes(vx * gain_ref[:, slab_cols(j)])
        each(n_ctx, lambda k: gc_copy(g, k, ctx).start())
        if g:
            blocks_summed(g - 1)

    mean = jnp.sum(macc, -1, keepdims=True) / D

    def write(j, _):
        cols = slab_cols(j)
        res = (gain_ref[:, cols] * ng[j] - xh[j] * mean) * inv_v[:, :1]
        out_v[:, cols] = res.astype(BF16)
        return 0

    lax.fori_loop(0, slabs, write, 0)
    out_copy = pltpu.make_async_copy(out_v, out_hbm, out_sem)
    out_copy.start()

    blocks_summed(groups - 1)

    for copy in halos:
        copy.wait_send()
    each(n_ctx, lambda k: tb_copy(k, ctx).wait_send())
    for g in range(groups):
        each(n_ctx, lambda k: gc_copy(g, k, ctx).wait_send())

    for p in range(n_tp - 1):
        for d in range(2):
            r = chunk[d][p]

            @pl.when(sends(d, r))
            def _():
                lax.fori_loop(0, slabs, lambda j, _: (rs_copy(d, r, j).wait_send(), 0)[1], 0)

    for g in range(groups):
        each(n_tp, lambda k: gt_copy(g, k, lax.rem(tp + k, n_tp)).wait_recv())
        gain_sum = sum(gain_tp[g, i] for i in range(n_tp))
        for i in range(per_group):
            j = g * per_group + i
            gain_out[:, j * slab_w:(j + 1) * slab_w] = gain_sum[i:i + 1]
    for g in range(groups):
        each(n_tp, lambda k: gt_copy(g, k, tp).wait_send())
    out_copy.wait()


def publish(*refs):
    for src, dst in zip(refs[:4], refs[4:]):
        dst[...] = src[...]


def on_device(n_ctx, n_tp, hidden_in, norm_gain, proj_weight, conv_in, conv_weight, conv_bias, act_grad):
    T, C = conv_in.shape
    D = proj_weight.shape[0]
    rows = hidden_in.shape[0]
    taps = conv_weight.shape[0]
    slab_w = D // 8
    slabs = D // slab_w
    groups = 4
    hbm = pl.BlockSpec(memory_space=pl.ANY)
    vmem = pl.BlockSpec(memory_space=pltpu.VMEM)
    dma = pltpu.SemaphoreType.DMA
    out_shape = (
        jax.ShapeDtypeStruct((rows, D), BF16),
        jax.ShapeDtypeStruct((1, D), F32),
        jax.ShapeDtypeStruct((taps, C), F32),
        jax.ShapeDtypeStruct((1, C), F32),
    )
    results = pl.pallas_call(
        functools.partial(kernel, n_ctx, n_tp, slab_w),
        out_shape=out_shape,
        in_specs=[hbm] * 7,
        out_specs=(hbm, vmem, vmem, vmem),
        scratch_shapes=[
            pltpu.VMEM((rows, D), BF16),
            pltpu.VMEM((D, C), BF16),
            pltpu.VMEM((T, C), BF16),
            pltpu.VMEM((T, C), BF16),
            pltpu.VMEM((1, D), F32),
            pltpu.VMEM((taps, C), F32),
            pltpu.VMEM((1, C), F32),
            pltpu.VMEM((3, EDGE, C), BF16),
            pltpu.VMEM((T + 2 * PAD, C), F32),
            pltpu.VMEM((T + PAD, C), F32),
            pltpu.VMEM((T - 2 * rows, C), BF16),
            pltpu.VMEM((2 * rows, C), BF16),
            pltpu.VMEM((8, C), F32),
            pltpu.VMEM((slabs, T, slab_w), F32),
            pltpu.VMEM((2, n_tp, slabs, rows, slab_w), BF16),
            pltpu.VMEM((2, n_tp, slabs, rows, slab_w), BF16),
            pltpu.VMEM((slabs, rows, slab_w), F32),
            pltpu.VMEM((slabs, rows, slab_w), F32),
            pltpu.VMEM((rows, LANES), F32),
            pltpu.VMEM((rows, D), BF16),
            pltpu.VMEM((n_ctx, 8, C), F32),
            pltpu.VMEM((groups, n_ctx, slabs // groups, slab_w), F32),
            pltpu.VMEM((groups, n_tp, slabs // groups, slab_w), F32),
            dma((6,)),
            dma((slabs,)),
            dma,
            dma((3,)),
            dma((3,)),
            dma((2, n_tp, slabs)),
            dma((2, n_tp, slabs)),
            dma((n_ctx,)),
            dma((n_ctx,)),
            dma((groups, n_ctx)),
            dma((groups, n_ctx)),
            dma((groups, n_tp)),
            dma((groups, n_tp)),
        ],
        compiler_params=pltpu.CompilerParams(
            collective_id=0, has_side_effects=True, vmem_limit_bytes=60 * 1024 * 1024
        ),
    )(
        hidden_in, norm_gain[None, :], proj_weight, conv_in, conv_weight, conv_bias[None, :], act_grad
    )
    grad, gain, taps_grad, bias_grad = pl.pallas_call(
        publish, out_shape=out_shape, in_specs=[vmem] * 4, out_specs=(vmem,) * 4
    )(*results)
    return grad, gain.reshape(-1), taps_grad, bias_grad.reshape(-1)


def solution(mesh):
    return jax.shard_map(
        functools.partial(on_device, mesh.shape["ctx"], mesh.shape["tp"]),
        mesh=mesh,
        in_specs=(
            P(("ctx", "tp"), None),
            P(),
            P(None, "tp"),
            P("ctx", "tp"),
            P(None, "tp"),
            P("tp"),
            P("ctx", "tp"),
        ),
        out_specs=(P(("ctx", "tp"), None), P(), P(None, "tp"), P("tp")),
        check_vma=False,
    )
```

```python
import functools

import jax
import jax.numpy as jnp
from jax import lax
from jax.experimental import pallas as pl
from jax.experimental.pallas import tpu as pltpu
from jax.sharding import PartitionSpec as P

MESH = pl.DeviceIdType.MESH
F32 = jnp.float32
BF16 = jnp.bfloat16
LANES = 128
EDGE = 16
PAD = 8
WINDOW = 3
LAG = 2


def chunk_of(rows, most=64):
    return max(r for r in range(EDGE, most + 1, EDGE) if rows % r == 0)


def each(count, body):
    if count <= 8:
        for k in range(1, count):
            body(k)
    else:
        lax.fori_loop(1, count, lambda k, _: (body(k), 0)[1], 0)


def kernel(
    n_ctx, n_tp, slab_w,
    hid_hbm, gain_hbm, w_hbm, x_hbm, taps_hbm, bias_hbm, g_hbm,
    out_hbm, gain_out, taps_out, bias_out,
    hid_v, w_v, x_v, g_v, gain_ref, taps_ref, bias_ref, halo, xf, pg, act_mid, act_edge, tb, prod, send, recv,
    xh, ng, inv_v, out_v, tb_all, gain_all, gain_tp,
    in_sem, w_sem, out_sem, halo_send, halo_recv, rs_send, rs_recv,
    tb_send, tb_recv, gc_send, gc_recv, gt_send, gt_recv,
):
    ctx = lax.axis_index("ctx")
    tp = lax.axis_index("tp")
    T, C = x_v.shape
    D = w_v.shape[0]
    taps = taps_ref.shape[0]
    rows = T // n_tp
    slabs = D // slab_w
    groups, _, per_group, _ = gain_all.shape
    prev_c, next_c = lax.rem(ctx + n_ctx - 1, n_ctx), lax.rem(ctx + 1, n_ctx)
    line = (lax.rem(tp + 1, n_tp), lax.rem(tp + n_tp - 1, n_tp))

    barrier = pltpu.get_barrier_semaphore()

    def greet_ctx(k):
        pl.semaphore_signal(barrier, inc=1, device_id={"ctx": lax.rem(ctx + k, n_ctx)}, device_id_type=MESH)

    def greet_tp(k):
        pl.semaphore_signal(barrier, inc=1, device_id={"tp": lax.rem(tp + k, n_tp)}, device_id_type=MESH)

    each(n_ctx, greet_ctx)
    each(n_tp, greet_tp)

    inputs = [
        pltpu.make_async_copy(src, dst, in_sem.at[i])
        for i, (src, dst) in enumerate([
            (x_hbm, x_v), (taps_hbm, taps_ref), (bias_hbm, bias_ref), (g_hbm, g_v),
            (hid_hbm, hid_v), (gain_hbm, gain_ref),
        ])
    ]
    for copy in inputs[:4]:
        copy.start()

    def w_copy(j):
        part = pl.ds(pl.multiple_of(j * slab_w, slab_w), slab_w)
        return pltpu.make_async_copy(w_hbm.at[part], w_v.at[part], w_sem.at[j])

    for j in range(slabs):
        w_copy(j).start()
    for copy in inputs[4:]:
        copy.start()

    def remote(src, dst, s_sem, r_sem, **where):
        return pltpu.make_async_remote_copy(
            src_ref=src, dst_ref=dst, send_sem=s_sem, recv_sem=r_sem,
            device_id=where, device_id_type=MESH,
        )

    def fold(v):
        return v.reshape(v.shape[0] // 8, 8, v.shape[1]).sum(0)

    def convert(t0, count, cols):
        xf[pl.ds(PAD + t0, count), cols] = x_v[pl.ds(t0, count), cols].astype(F32)

    def grad_rows(t0, count, cols, cot):
        pre = bias_ref[:, cols] + sum(
            taps_ref[pl.ds(k, 1), cols] * xf[pl.ds(PAD + t0 - k, count), cols] for k in range(taps)
        )
        s = 0.5 * jnp.tanh(0.5 * pre) + 0.5
        return cot.astype(F32) * s * (1.0 + pre * (1.0 - s))

    def own_grad(first, stop, cols):
        step = chunk_of(stop - first)
        for t0 in range(first, stop, step):
            pg[pl.ds(t0, step), cols] = grad_rows(t0, step, cols, g_v[pl.ds(t0, step), cols])

    def in_rows(dst, at, first, count, cols):
        step = chunk_of(count)
        for i in range(0, count, step):
            total = sum(
                taps_ref[pl.ds(k, 1), cols] * pg[pl.ds(first + i + k, step), cols] for k in range(taps)
            )
            dst[pl.ds(at + i, step), cols] = total.astype(BF16)

    def columns(c):
        return pl.ds(pl.multiple_of(c * LANES, LANES), LANES)

    for copy in inputs[:4]:
        copy.wait()

    def middle(c, _):
        cols = columns(c)
        convert(rows - EDGE, T - 2 * rows + 2 * EDGE, cols)
        own_grad(rows, T - rows + EDGE, cols)
        in_rows(act_mid, 0, rows, T - 2 * rows, cols)
        return 0

    lax.fori_loop(0, C // LANES, middle, 0)

    pl.semaphore_wait(barrier, n_ctx + n_tp - 2)
    halos = [
        remote(x_hbm.at[pl.ds(T - EDGE, EDGE)], halo.at[0], halo_send.at[0], halo_recv.at[0], ctx=next_c),
        remote(x_hbm.at[pl.ds(0, EDGE)], halo.at[1], halo_send.at[1], halo_recv.at[1], ctx=prev_c),
        remote(g_hbm.at[pl.ds(0, EDGE)], halo.at[2], halo_send.at[2], halo_recv.at[2], ctx=prev_c),
    ]
    for copy in halos:
        copy.start()

    up = [n_tp - 2, n_tp - 1] + list(range(n_tp - 3, 0, -1))
    chunk = (up, [n_tp - 1 - r for r in up])
    begins = (tp == 0, tp == n_tp - 1)

    def sends(d, r):
        return tp < r if d == 0 else tp > r

    def rs_copy(d, r, j):
        return remote(
            send.at[d, r, j], recv.at[d, r, j], rs_send.at[d, r, j], rs_recv.at[d, r, j],
            tp=line[d],
        )

    def term(r, j):
        return prod[j, pl.ds(r * rows, rows), :]

    def begin(p, j):
        for d in range(2):
            r = chunk[d][p]

            @pl.when(begins[d])
            def _():
                send[d, r, j] = term(r, j).astype(BF16)
                if p == 0:
                    pl.when(j >= WINDOW)(lambda: rs_copy(d, r, j - WINDOW).wait_send())
                else:
                    old = jnp.where(j >= WINDOW, r, chunk[d][p - 1])
                    rs_copy(d, old, lax.rem(j + slabs - WINDOW, slabs)).wait_send()
                rs_copy(d, r, j).start()

    def dot(a, j):
        part = pl.ds(pl.multiple_of(j * slab_w, slab_w), slab_w)
        return lax.dot_general(
            a[...], w_v[part, :], (((1,), (1,)), ((), ())), preferred_element_type=F32
        )

    def middle_dot(j, _):
        w_copy(j).wait()
        prod[j, pl.ds(rows, T - 2 * rows), :] = dot(act_mid, j)
        begin(0, j)
        return 0

    lax.fori_loop(0, slabs, middle_dot, 0)

    for copy in halos:
        copy.wait_recv()
    has_prev = (ctx > 0).astype(F32)
    has_next = (ctx < n_ctx - 1).astype(F32)

    def edges(c, _):
        cols = columns(c)
        xf[pl.ds(0, PAD), cols] = halo[0, :, cols].astype(F32)[EDGE - PAD:] * has_prev
        xf[pl.ds(PAD + T, PAD), cols] = halo[1, :, cols].astype(F32)[:PAD]
        convert(0, rows - EDGE, cols)
        convert(T - rows + EDGE, rows - EDGE, cols)
        own_grad(0, rows, cols)
        own_grad(T - rows + EDGE, T, cols)
        pg[pl.ds(T, PAD), cols] = has_next * grad_rows(T, PAD, cols, halo[2, :, cols].astype(F32)[:PAD])
        in_rows(act_edge, 0, 0, rows, cols)
        in_rows(act_edge, rows, T - rows, rows, cols)
        return 0

    lax.fori_loop(0, C // LANES, edges, 0)

    def edge_dot(j, _):
        both = dot(act_edge, j)
        prod[j, pl.ds(0, rows), :] = both[:rows]
        prod[j, pl.ds(T - rows, rows), :] = both[rows:]
        begin(1, j)
        return 0

    lax.fori_loop(0, slabs, edge_dot, 0)

    tb[...] = jnp.zeros_like(tb)

    def taps_terms(c, _):
        cols = columns(c)
        sums = [jnp.zeros((8, LANES), F32) for _ in range(taps + 1)]
        step = chunk_of(T)
        for t0 in range(0, T, step):
            g = pg[pl.ds(t0, step), cols]
            for k in range(taps):
                sums[k] += fold(g * xf[pl.ds(PAD + t0 - k, step), cols])
            sums[taps] += fold(g)
        for k in range(taps + 1):
            tb[pl.ds(k, 1), cols] = jnp.sum(sums[k], 0, keepdims=True)
        return 0

    lax.fori_loop(0, C // LANES, taps_terms, 0)
    tb_all[ctx] = tb[...]

    def tb_copy(k, slot):
        return remote(
            tb_all.at[slot], tb_all.at[slot], tb_send.at[k], tb_recv.at[slot],
            ctx=lax.rem(ctx + k, n_ctx),
        )

    each(n_ctx, lambda k: tb_copy(k, ctx).start())

    for copy in inputs[4:]:
        copy.wait()

    def slab_cols(j):
        return pl.ds(pl.multiple_of(j * slab_w, slab_w), slab_w)

    def fold_lanes(v):
        return sum(v[:, i:i + LANES] for i in range(0, v.shape[1], LANES))

    def squares(j, acc):
        h = hid_v[:, slab_cols(j)].astype(F32)
        return acc + fold_lanes(h * h)

    acc = lax.fori_loop(0, slabs, squares, jnp.zeros((rows, LANES), F32))
    inv = lax.rsqrt(jnp.sum(acc, -1, keepdims=True) / D + 1e-05)
    inv_v[...] = jnp.broadcast_to(inv, (rows, LANES))

    def normalise(j, _):
        xh[j] = hid_v[:, slab_cols(j)].astype(F32) * inv_v[:, :1]
        return 0

    lax.fori_loop(0, slabs, normalise, 0)

    def later_begin(j, _, p=2):
        begin(p, j)
        return 0

    for p in range(2, n_tp - 1):
        lax.fori_loop(0, slabs, functools.partial(later_begin, p=p), 0)

    lower = 2 * tp < n_tp

    def forward(i, _, p=0):
        def one(d, j, now):
            r = chunk[d][p]

            @pl.when(now & sends(d, r) & jnp.logical_not(begins[d]))
            def _():
                rs_copy(d, r, j).wait_recv()
                send[d, r, j] = (term(r, j) + recv[d, r, j].astype(F32)).astype(BF16)
                rs_copy(d, r, j).start()

        upper = jnp.logical_not(lower)
        one(0, i, lower & (i < slabs))
        one(1, i, upper & (i < slabs))
        one(1, i - LAG, lower & (i >= LAG))
        one(0, i - LAG, upper & (i >= LAG))
        return 0

    for p in range(n_tp - 1):
        lax.fori_loop(0, slabs + LAG, functools.partial(forward, p=p), 0)

    each(n_ctx, lambda k: tb_copy(k, lax.rem(ctx + k, n_ctx)).wait_recv())
    total = lax.fori_loop(1, n_ctx, lambda i, t: t + tb_all[i], tb_all[0])
    taps_out[...] = total[:taps]
    bias_out[...] = total[taps:taps + 1]

    def gc_copy(g, k, slot):
        return remote(
            gain_all.at[g, slot], gain_all.at[g, slot], gc_send.at[g, k], gc_recv.at[g, slot],
            ctx=lax.rem(ctx + k, n_ctx),
        )

    def gt_copy(g, k, slot):
        return remote(
            gain_tp.at[g, slot], gain_tp.at[g, slot], gt_send.at[g, k], gt_recv.at[g, slot],
            tp=lax.rem(tp + k, n_tp),
        )

    def blocks_summed(g):
        each(n_ctx, lambda k: gc_copy(g, k, lax.rem(ctx + k, n_ctx)).wait_recv())
        gain_tp[g, tp] = lax.fori_loop(1, n_ctx, lambda i, t: t + gain_all[g, i], gain_all[g, 0])
        each(n_tp, lambda k: gt_copy(g, k, tp).start())

    macc = jnp.zeros((rows, LANES), F32)
    for g in range(groups):
        for i in range(per_group):
            j = g * per_group + i
            ng[j] = prod[j, pl.ds(pl.multiple_of(tp * rows, rows), rows), :]

            def arrived(d):
                rs_copy(d, tp, j).wait_recv()
                ng[j] = ng[j] + recv[d, tp, j].astype(F32)

            pl.when(tp < n_tp - 1)(functools.partial(arrived, 1))
            pl.when(tp > 0)(functools.partial(arrived, 0))
            vx = ng[j] * xh[j]
            gain_all[g, ctx, pl.ds(i, 1), :] = jnp.sum(fold(vx), 0, keepdims=True)
            macc = macc + fold_lanes(vx * gain_ref[:, slab_cols(j)])
        each(n_ctx, lambda k: gc_copy(g, k, ctx).start())
        if g:
            blocks_summed(g - 1)

    mean = jnp.sum(macc, -1, keepdims=True) / D

    def write(j, _):
        cols = slab_cols(j)
        res = (gain_ref[:, cols] * ng[j] - xh[j] * mean) * inv_v[:, :1]
        out_v[:, cols] = res.astype(BF16)
        return 0

    lax.fori_loop(0, slabs, write, 0)
    out_copy = pltpu.make_async_copy(out_v, out_hbm, out_sem)
    out_copy.start()

    blocks_summed(groups - 1)

    for copy in halos:
        copy.wait_send()
    each(n_ctx, lambda k: tb_copy(k, ctx).wait_send())
    for g in range(groups):
        each(n_ctx, lambda k: gc_copy(g, k, ctx).wait_send())

    for d in range(2):
        @pl.when(begins[d])
        def _():
            for j in range(slabs - WINDOW, slabs):
                rs_copy(d, chunk[d][-1], j).wait_send()

    for p in range(n_tp - 1):
        for d in range(2):
            r = chunk[d][p]

            @pl.when(sends(d, r) & jnp.logical_not(begins[d]))
            def _():
                lax.fori_loop(0, slabs, lambda j, _: (rs_copy(d, r, j).wait_send(), 0)[1], 0)

    for g in range(groups):
        each(n_tp, lambda k: gt_copy(g, k, lax.rem(tp + k, n_tp)).wait_recv())
        gain_sum = sum(gain_tp[g, i] for i in range(n_tp))
        for i in range(per_group):
            j = g * per_group + i
            gain_out[:, j * slab_w:(j + 1) * slab_w] = gain_sum[i:i + 1]
    for g in range(groups):
        each(n_tp, lambda k: gt_copy(g, k, tp).wait_send())
    out_copy.wait()


def publish(*refs):
    for src, dst in zip(refs[:4], refs[4:]):
        dst[...] = src[...]


def on_device(n_ctx, n_tp, hidden_in, norm_gain, proj_weight, conv_in, conv_weight, conv_bias, act_grad):
    T, C = conv_in.shape
    D = proj_weight.shape[0]
    rows = hidden_in.shape[0]
    taps = conv_weight.shape[0]
    slab_w = D // 8
    slabs = D // slab_w
    groups = 4
    hbm = pl.BlockSpec(memory_space=pl.ANY)
    vmem = pl.BlockSpec(memory_space=pltpu.VMEM)
    dma = pltpu.SemaphoreType.DMA
    out_shape = (
        jax.ShapeDtypeStruct((rows, D), BF16),
        jax.ShapeDtypeStruct((1, D), F32),
        jax.ShapeDtypeStruct((taps, C), F32),
        jax.ShapeDtypeStruct((1, C), F32),
    )
    results = pl.pallas_call(
        functools.partial(kernel, n_ctx, n_tp, slab_w),
        out_shape=out_shape,
        in_specs=[hbm] * 7,
        out_specs=(hbm, vmem, vmem, vmem),
        scratch_shapes=[
            pltpu.VMEM((rows, D), BF16),
            pltpu.VMEM((D, C), BF16),
            pltpu.VMEM((T, C), BF16),
            pltpu.VMEM((T, C), BF16),
            pltpu.VMEM((1, D), F32),
            pltpu.VMEM((taps, C), F32),
            pltpu.VMEM((1, C), F32),
            pltpu.VMEM((3, EDGE, C), BF16),
            pltpu.VMEM((T + 2 * PAD, C), F32),
            pltpu.VMEM((T + PAD, C), F32),
            pltpu.VMEM((T - 2 * rows, C), BF16),
            pltpu.VMEM((2 * rows, C), BF16),
            pltpu.VMEM((8, C), F32),
            pltpu.VMEM((slabs, T, slab_w), F32),
            pltpu.VMEM((2, n_tp, slabs, rows, slab_w), BF16),
            pltpu.VMEM((2, n_tp, slabs, rows, slab_w), BF16),
            pltpu.VMEM((slabs, rows, slab_w), F32),
            pltpu.VMEM((slabs, rows, slab_w), F32),
            pltpu.VMEM((rows, LANES), F32),
            pltpu.VMEM((rows, D), BF16),
            pltpu.VMEM((n_ctx, 8, C), F32),
            pltpu.VMEM((groups, n_ctx, slabs // groups, slab_w), F32),
            pltpu.VMEM((groups, n_tp, slabs // groups, slab_w), F32),
            dma((6,)),
            dma((slabs,)),
            dma,
            dma((3,)),
            dma((3,)),
            dma((2, n_tp, slabs)),
            dma((2, n_tp, slabs)),
            dma((n_ctx,)),
            dma((n_ctx,)),
            dma((groups, n_ctx)),
            dma((groups, n_ctx)),
            dma((groups, n_tp)),
            dma((groups, n_tp)),
        ],
        compiler_params=pltpu.CompilerParams(
            collective_id=0, has_side_effects=True, vmem_limit_bytes=60 * 1024 * 1024
        ),
    )(
        hidden_in, norm_gain[None, :], proj_weight, conv_in, conv_weight, conv_bias[None, :], act_grad
    )
    grad, gain, taps_grad, bias_grad = pl.pallas_call(
        publish, out_shape=out_shape, in_specs=[vmem] * 4, out_specs=(vmem,) * 4
    )(*results)
    return grad, gain.reshape(-1), taps_grad, bias_grad.reshape(-1)


def solution(mesh):
    return jax.shard_map(
        functools.partial(on_device, mesh.shape["ctx"], mesh.shape["tp"]),
        mesh=mesh,
        in_specs=(
            P(("ctx", "tp"), None),
            P(),
            P(None, "tp"),
            P("ctx", "tp"),
            P(None, "tp"),
            P("tp"),
            P("ctx", "tp"),
        ),
        out_specs=(P(("ctx", "tp"), None), P(), P(None, "tp"), P("tp")),
        check_vma=False,
    )
```

```python
import functools

import jax
import jax.numpy as jnp
from jax import lax
from jax.experimental import pallas as pl
from jax.experimental.pallas import tpu as pltpu
from jax.sharding import PartitionSpec as P

MESH = pl.DeviceIdType.MESH
F32 = jnp.float32
BF16 = jnp.bfloat16
LANES = 128
EDGE = 16
PAD = 8
WINDOW = 3
LAG = 2


def chunk_of(rows, most=64):
    return max(r for r in range(EDGE, most + 1, EDGE) if rows % r == 0)


def each(count, body):
    if count <= 8:
        for k in range(1, count):
            body(k)
    else:
        lax.fori_loop(1, count, lambda k, _: (body(k), 0)[1], 0)


def kernel(
    n_ctx, n_tp, slab_w,
    hid_hbm, gain_hbm, w_hbm, x_hbm, taps_hbm, bias_hbm, g_hbm,
    out_hbm, gain_out, taps_out, bias_out,
    hid_v, w_v, x_v, g_v, gain_ref, taps_ref, bias_ref, halo, xf, pg, act_mid, act_edge, tb, prod, send, recv,
    xh, ng, inv_v, out_v, tb_all, gain_all, gain_tp,
    in_sem, w_sem, out_sem, halo_send, halo_recv, rs_send, rs_recv,
    tb_send, tb_recv, gc_send, gc_recv, gt_send, gt_recv,
):
    ctx = lax.axis_index("ctx")
    tp = lax.axis_index("tp")
    T, C = x_v.shape
    D = w_v.shape[0]
    taps = taps_ref.shape[0]
    rows = T // n_tp
    slabs = D // slab_w
    groups, _, per_group, _ = gain_all.shape
    prev_c, next_c = lax.rem(ctx + n_ctx - 1, n_ctx), lax.rem(ctx + 1, n_ctx)
    line = (lax.rem(tp + 1, n_tp), lax.rem(tp + n_tp - 1, n_tp))

    barrier = pltpu.get_barrier_semaphore()

    def greet_ctx(k):
        pl.semaphore_signal(barrier, inc=1, device_id={"ctx": lax.rem(ctx + k, n_ctx)}, device_id_type=MESH)

    def greet_tp(k):
        pl.semaphore_signal(barrier, inc=1, device_id={"tp": lax.rem(tp + k, n_tp)}, device_id_type=MESH)

    each(n_ctx, greet_ctx)
    each(n_tp, greet_tp)

    inputs = [
        pltpu.make_async_copy(src, dst, in_sem.at[i])
        for i, (src, dst) in enumerate([
            (x_hbm, x_v), (taps_hbm, taps_ref), (bias_hbm, bias_ref), (g_hbm, g_v),
            (hid_hbm, hid_v), (gain_hbm, gain_ref),
        ])
    ]
    for copy in inputs[:4]:
        copy.start()

    def w_copy(j):
        part = pl.ds(pl.multiple_of(j * slab_w, slab_w), slab_w)
        return pltpu.make_async_copy(w_hbm.at[part], w_v.at[part], w_sem.at[j])

    def remote(src, dst, s_sem, r_sem, **where):
        return pltpu.make_async_remote_copy(
            src_ref=src, dst_ref=dst, send_sem=s_sem, recv_sem=r_sem,
            device_id=where, device_id_type=MESH,
        )

    def fold(v):
        return v.reshape(v.shape[0] // 8, 8, v.shape[1]).sum(0)

    def convert(t0, count, cols):
        xf[pl.ds(PAD + t0, count), cols] = x_v[pl.ds(t0, count), cols].astype(F32)

    def grad_rows(t0, count, cols, cot):
        pre = bias_ref[:, cols] + sum(
            taps_ref[pl.ds(k, 1), cols] * xf[pl.ds(PAD + t0 - k, count), cols] for k in range(taps)
        )
        s = 0.5 * jnp.tanh(0.5 * pre) + 0.5
        return cot.astype(F32) * s * (1.0 + pre * (1.0 - s))

    def own_grad(first, stop, cols):
        step = chunk_of(stop - first)
        for t0 in range(first, stop, step):
            pg[pl.ds(t0, step), cols] = grad_rows(t0, step, cols, g_v[pl.ds(t0, step), cols])

    def in_rows(dst, at, first, count, cols):
        step = chunk_of(count)
        for i in range(0, count, step):
            total = sum(
                taps_ref[pl.ds(k, 1), cols] * pg[pl.ds(first + i + k, step), cols] for k in range(taps)
            )
            dst[pl.ds(at + i, step), cols] = total.astype(BF16)

    def columns(c):
        return pl.ds(pl.multiple_of(c * LANES, LANES), LANES)

    for copy in inputs[:4]:
        copy.wait()
    for j in range(slabs):
        w_copy(j).start()
    for copy in inputs[4:]:
        copy.start()

    def middle(c, _):
        cols = columns(c)
        convert(rows - EDGE, T - 2 * rows + 2 * EDGE, cols)
        own_grad(rows, T - rows + EDGE, cols)
        in_rows(act_mid, 0, rows, T - 2 * rows, cols)
        return 0

    lax.fori_loop(0, C // LANES, middle, 0)

    pl.semaphore_wait(barrier, n_ctx + n_tp - 2)
    halos = [
        remote(x_hbm.at[pl.ds(T - EDGE, EDGE)], halo.at[0], halo_send.at[0], halo_recv.at[0], ctx=next_c),
        remote(x_hbm.at[pl.ds(0, EDGE)], halo.at[1], halo_send.at[1], halo_recv.at[1], ctx=prev_c),
        remote(g_hbm.at[pl.ds(0, EDGE)], halo.at[2], halo_send.at[2], halo_recv.at[2], ctx=prev_c),
    ]
    for copy in halos:
        copy.start()

    up = [n_tp - 2, n_tp - 1] + list(range(n_tp - 3, 0, -1))
    chunk = (up, [n_tp - 1 - r for r in up])
    begins = (tp == 0, tp == n_tp - 1)

    def sends(d, r):
        return tp < r if d == 0 else tp > r

    def rs_copy(d, r, j):
        return remote(
            send.at[d, r, j], recv.at[d, r, j], rs_send.at[d, r, j], rs_recv.at[d, r, j],
            tp=line[d],
        )

    def term(r, j):
        return prod[j, pl.ds(r * rows, rows), :]

    def begin(p, j):
        for d in range(2):
            r = chunk[d][p]

            @pl.when(begins[d])
            def _():
                send[d, r, j] = term(r, j).astype(BF16)
                if p == 0:
                    pl.when(j >= WINDOW)(lambda: rs_copy(d, r, j - WINDOW).wait_send())
                else:
                    earlier = chunk[d][p - 1]
                    if isinstance(j, int):
                        old = r if j >= WINDOW else earlier
                        rs_copy(d, old, (j - WINDOW) % slabs).wait_send()
                    else:
                        old = jnp.where(j >= WINDOW, r, earlier)
                        rs_copy(d, old, lax.rem(j + slabs - WINDOW, slabs)).wait_send()
                rs_copy(d, r, j).start()

    def pass_on(d, p, j, now=True):
        r = chunk[d][p]

        @pl.when(now & sends(d, r) & jnp.logical_not(begins[d]))
        def _():
            rs_copy(d, r, j).wait_recv()
            send[d, r, j] = (term(r, j) + recv[d, r, j].astype(F32)).astype(BF16)
            rs_copy(d, r, j).start()

    def forward(i, _, p=0):
        lower = 2 * tp < n_tp
        upper = jnp.logical_not(lower)
        pass_on(0, p, i, lower & (i < slabs))
        pass_on(1, p, i, upper & (i < slabs))
        pass_on(1, p, i - LAG, lower & (i >= LAG))
        pass_on(0, p, i - LAG, upper & (i >= LAG))
        return 0

    def dot(a, j):
        part = pl.ds(pl.multiple_of(j * slab_w, slab_w), slab_w)
        return lax.dot_general(
            a[...], w_v[part, :], (((1,), (1,)), ((), ())), preferred_element_type=F32
        )

    def middle_dot(j, _):
        w_copy(j).wait()
        prod[j, pl.ds(rows, T - 2 * rows), :] = dot(act_mid, j)
        begin(0, j)
        return 0

    lax.fori_loop(0, slabs, middle_dot, 0)

    for copy in halos:
        copy.wait_recv()
    has_prev = (ctx > 0).astype(F32)
    has_next = (ctx < n_ctx - 1).astype(F32)

    def edges(c, _):
        cols = columns(c)
        xf[pl.ds(0, PAD), cols] = halo[0, :, cols].astype(F32)[EDGE - PAD:] * has_prev
        xf[pl.ds(PAD + T, PAD), cols] = halo[1, :, cols].astype(F32)[:PAD]
        convert(0, rows - EDGE, cols)
        convert(T - rows + EDGE, rows - EDGE, cols)
        own_grad(0, rows, cols)
        own_grad(T - rows + EDGE, T, cols)
        pg[pl.ds(T, PAD), cols] = has_next * grad_rows(T, PAD, cols, halo[2, :, cols].astype(F32)[:PAD])
        in_rows(act_edge, 0, 0, rows, cols)
        in_rows(act_edge, rows, T - rows, rows, cols)
        return 0

    lax.fori_loop(0, C // LANES, edges, 0)

    def edge_dot(j, _):
        both = dot(act_edge, j)
        prod[j, pl.ds(0, rows), :] = both[:rows]
        prod[j, pl.ds(T - rows, rows), :] = both[rows:]
        begin(1, j)
        pass_on(0, 0, j)
        pass_on(1, 0, j)
        return 0

    lax.fori_loop(0, slabs, edge_dot, 0)

    tb[...] = jnp.zeros_like(tb)

    def taps_terms(c, _):
        cols = columns(c)
        sums = [jnp.zeros((8, LANES), F32) for _ in range(taps + 1)]
        step = chunk_of(T)
        for t0 in range(0, T, step):
            g = pg[pl.ds(t0, step), cols]
            for k in range(taps):
                sums[k] += fold(g * xf[pl.ds(PAD + t0 - k, step), cols])
            sums[taps] += fold(g)
        for k in range(taps + 1):
            tb[pl.ds(k, 1), cols] = jnp.sum(sums[k], 0, keepdims=True)
        return 0

    lax.fori_loop(0, C // LANES, taps_terms, 0)
    tb_all[ctx] = tb[...]

    def tb_copy(k, slot):
        return remote(
            tb_all.at[slot], tb_all.at[slot], tb_send.at[k], tb_recv.at[slot],
            ctx=lax.rem(ctx + k, n_ctx),
        )

    each(n_ctx, lambda k: tb_copy(k, ctx).start())

    for copy in inputs[4:]:
        copy.wait()

    def slab_cols(j):
        return pl.ds(pl.multiple_of(j * slab_w, slab_w), slab_w)

    def fold_lanes(v):
        return sum(v[:, i:i + LANES] for i in range(0, v.shape[1], LANES))

    def squares(j, acc):
        h = hid_v[:, slab_cols(j)].astype(F32)
        return acc + fold_lanes(h * h)

    acc = lax.fori_loop(0, slabs, squares, jnp.zeros((rows, LANES), F32))
    inv = lax.rsqrt(jnp.sum(acc, -1, keepdims=True) / D + 1e-05)
    inv_v[...] = jnp.broadcast_to(inv, (rows, LANES))

    def normalise(j, _):
        xh[j] = hid_v[:, slab_cols(j)].astype(F32) * inv_v[:, :1]
        return 0

    lax.fori_loop(0, slabs, normalise, 0)

    def later_begin(j, _, p=2):
        begin(p, j)
        return 0

    for p in range(2, n_tp - 2):
        lax.fori_loop(0, slabs, functools.partial(later_begin, p=p), 0)

    for p in range(1, n_tp - 2):
        lax.fori_loop(0, slabs + LAG, functools.partial(forward, p=p), 0)

    def gc_copy(g, k, slot):
        return remote(
            gain_all.at[g, slot], gain_all.at[g, slot], gc_send.at[g, k], gc_recv.at[g, slot],
            ctx=lax.rem(ctx + k, n_ctx),
        )

    def gt_copy(g, k, slot):
        return remote(
            gain_tp.at[g, slot], gain_tp.at[g, slot], gt_send.at[g, k], gt_recv.at[g, slot],
            tp=lax.rem(tp + k, n_tp),
        )

    def blocks_summed(g):
        each(n_ctx, lambda k: gc_copy(g, k, lax.rem(ctx + k, n_ctx)).wait_recv())
        gain_tp[g, tp] = lax.fori_loop(1, n_ctx, lambda i, t: t + gain_all[g, i], gain_all[g, 0])
        each(n_tp, lambda k: gt_copy(g, k, tp).start())

    macc = jnp.zeros((rows, LANES), F32)
    for g in range(groups):
        for i in range(per_group):
            j = g * per_group + i
            begin(n_tp - 2, j)
            ng[j] = prod[j, pl.ds(pl.multiple_of(tp * rows, rows), rows), :]

            def arrived(d):
                rs_copy(d, tp, j).wait_recv()
                ng[j] = ng[j] + recv[d, tp, j].astype(F32)

            pl.when(tp < n_tp - 1)(functools.partial(arrived, 1))
            pl.when(tp > 0)(functools.partial(arrived, 0))
            vx = ng[j] * xh[j]
            gain_all[g, ctx, pl.ds(i, 1), :] = jnp.sum(fold(vx), 0, keepdims=True)
            macc = macc + fold_lanes(vx * gain_ref[:, slab_cols(j)])
        each(n_ctx, lambda k: gc_copy(g, k, ctx).start())
        if g:
            blocks_summed(g - 1)

    mean = jnp.sum(macc, -1, keepdims=True) / D

    def write(j, _):
        cols = slab_cols(j)
        res = (gain_ref[:, cols] * ng[j] - xh[j] * mean) * inv_v[:, :1]
        out_v[:, cols] = res.astype(BF16)
        return 0

    lax.fori_loop(0, slabs, write, 0)
    out_copy = pltpu.make_async_copy(out_v, out_hbm, out_sem)
    out_copy.start()

    each(n_ctx, lambda k: tb_copy(k, lax.rem(ctx + k, n_ctx)).wait_recv())
    total = lax.fori_loop(1, n_ctx, lambda i, t: t + tb_all[i], tb_all[0])
    taps_out[...] = total[:taps]
    bias_out[...] = total[taps:taps + 1]

    blocks_summed(groups - 1)

    for copy in halos:
        copy.wait_send()
    each(n_ctx, lambda k: tb_copy(k, ctx).wait_send())
    for g in range(groups):
        each(n_ctx, lambda k: gc_copy(g, k, ctx).wait_send())

    for d in range(2):
        @pl.when(begins[d])
        def _():
            for j in range(slabs - WINDOW, slabs):
                rs_copy(d, chunk[d][-1], j).wait_send()

    for p in range(n_tp - 1):
        for d in range(2):
            r = chunk[d][p]

            @pl.when(sends(d, r) & jnp.logical_not(begins[d]))
            def _():
                lax.fori_loop(0, slabs, lambda j, _: (rs_copy(d, r, j).wait_send(), 0)[1], 0)

    for g in range(groups):
        each(n_tp, lambda k: gt_copy(g, k, lax.rem(tp + k, n_tp)).wait_recv())
        gain_sum = sum(gain_tp[g, i] for i in range(n_tp))
        for i in range(per_group):
            j = g * per_group + i
            gain_out[:, j * slab_w:(j + 1) * slab_w] = gain_sum[i:i + 1]
    for g in range(groups):
        each(n_tp, lambda k: gt_copy(g, k, tp).wait_send())
    out_copy.wait()


def publish(*refs):
    for src, dst in zip(refs[:4], refs[4:]):
        dst[...] = src[...]


def on_device(n_ctx, n_tp, hidden_in, norm_gain, proj_weight, conv_in, conv_weight, conv_bias, act_grad):
    T, C = conv_in.shape
    D = proj_weight.shape[0]
    rows = hidden_in.shape[0]
    taps = conv_weight.shape[0]
    slab_w = D // 8
    slabs = D // slab_w
    groups = 4
    hbm = pl.BlockSpec(memory_space=pl.ANY)
    vmem = pl.BlockSpec(memory_space=pltpu.VMEM)
    dma = pltpu.SemaphoreType.DMA
    out_shape = (
        jax.ShapeDtypeStruct((rows, D), BF16),
        jax.ShapeDtypeStruct((1, D), F32),
        jax.ShapeDtypeStruct((taps, C), F32),
        jax.ShapeDtypeStruct((1, C), F32),
    )
    results = pl.pallas_call(
        functools.partial(kernel, n_ctx, n_tp, slab_w),
        out_shape=out_shape,
        in_specs=[hbm] * 7,
        out_specs=(hbm, vmem, vmem, vmem),
        scratch_shapes=[
            pltpu.VMEM((rows, D), BF16),
            pltpu.VMEM((D, C), BF16),
            pltpu.VMEM((T, C), BF16),
            pltpu.VMEM((T, C), BF16),
            pltpu.VMEM((1, D), F32),
            pltpu.VMEM((taps, C), F32),
            pltpu.VMEM((1, C), F32),
            pltpu.VMEM((3, EDGE, C), BF16),
            pltpu.VMEM((T + 2 * PAD, C), F32),
            pltpu.VMEM((T + PAD, C), F32),
            pltpu.VMEM((T - 2 * rows, C), BF16),
            pltpu.VMEM((2 * rows, C), BF16),
            pltpu.VMEM((8, C), F32),
            pltpu.VMEM((slabs, T, slab_w), F32),
            pltpu.VMEM((2, n_tp, slabs, rows, slab_w), BF16),
            pltpu.VMEM((2, n_tp, slabs, rows, slab_w), BF16),
            pltpu.VMEM((slabs, rows, slab_w), F32),
            pltpu.VMEM((slabs, rows, slab_w), F32),
            pltpu.VMEM((rows, LANES), F32),
            pltpu.VMEM((rows, D), BF16),
            pltpu.VMEM((n_ctx, 8, C), F32),
            pltpu.VMEM((groups, n_ctx, slabs // groups, slab_w), F32),
            pltpu.VMEM((groups, n_tp, slabs // groups, slab_w), F32),
            dma((6,)),
            dma((slabs,)),
            dma,
            dma((3,)),
            dma((3,)),
            dma((2, n_tp, slabs)),
            dma((2, n_tp, slabs)),
            dma((n_ctx,)),
            dma((n_ctx,)),
            dma((groups, n_ctx)),
            dma((groups, n_ctx)),
            dma((groups, n_tp)),
            dma((groups, n_tp)),
        ],
        compiler_params=pltpu.CompilerParams(
            collective_id=0, has_side_effects=True, vmem_limit_bytes=60 * 1024 * 1024
        ),
    )(
        hidden_in, norm_gain[None, :], proj_weight, conv_in, conv_weight, conv_bias[None, :], act_grad
    )
    grad, gain, taps_grad, bias_grad = pl.pallas_call(
        publish, out_shape=out_shape, in_specs=[vmem] * 4, out_specs=(vmem,) * 4
    )(*results)
    return grad, gain.reshape(-1), taps_grad, bias_grad.reshape(-1)


def solution(mesh):
    return jax.shard_map(
        functools.partial(on_device, mesh.shape["ctx"], mesh.shape["tp"]),
        mesh=mesh,
        in_specs=(
            P(("ctx", "tp"), None),
            P(),
            P(None, "tp"),
            P("ctx", "tp"),
            P(None, "tp"),
            P("tp"),
            P("ctx", "tp"),
        ),
        out_specs=(P(("ctx", "tp"), None), P(), P(None, "tp"), P("tp")),
        check_vma=False,
    )
```
